32 devices in a mesh: dp: 1 (over z), tp: 4 (over y), sp: 8 (over x, core).
Axes of the slice: x: 4, y: 4, z: 1, core: 2. Of those that a mesh axis runs over, the one named last changes fastest.
The devices are a block of a 4x4x8 slice.
Arguments:
- k_cache: bfloat16 [4, 8, 4, 8192, 64], P(None, 'dp', 'tp', 'sp')
- v_cache: bfloat16 [4, 8, 4, 8192, 64], P(None, 'dp', 'tp', 'sp')
- lengths: int32 [8], P('dp')
- hidden: bfloat16 [8, 2048], P(('dp', 'sp'))
- ln_gain: bfloat16 [4, 2048], replicated
- w_query: bfloat16 [4, 2048, 2048], P(None, None, 'tp')
- w_key: bfloat16 [4, 2048, 256], P(None, None, 'tp')
- w_value: bfloat16 [4, 2048, 256], P(None, None, 'tp')
- w_out: bfloat16 [4, 2048, 2048], P(None, 'tp')
- w_gate: bfloat16 [4, 2048, 5632], P(None, None, 'tp')
- w_up: bfloat16 [4, 2048, 5632], P(None, None, 'tp')
- w_down: bfloat16 [4, 5632, 2048], P(None, 'tp')
Outputs:
- output 1: bfloat16 [8, 2048], P(('dp', 'sp'))
- output 2: bfloat16 [3, 8, 4, 4096, 64], P(None, ('dp', 'sp'), 'tp')
- output 3: bfloat16 [3, 8, 4, 4096, 64], P(None, ('dp', 'sp'), 'tp')
- output 4: bfloat16 [8, 4, 8192, 64], P(('dp', 'sp'), 'tp')
- output 5: bfloat16 [8, 4, 8192, 64], P(('dp', 'sp'), 'tp')
All inputs are finite; a program needn't handle non-finite values.
Results may differ from the reference program's by a relative error of at most 0.02.
Values are sent between devices in bfloat16 or wider.
A program may use at most 768 MiB of HBM per device.

```python
import jax
import jax.numpy as jnp
from jax import lax

N_ROWS = 8
SEQ_LEN = 8192
MODEL_DIM = 2048
N_HEADS = 32
KV_HEADS = 4
HEAD_DIM = 64
FFN_DIM = 5632
WINDOW = 4096
ROPE_BASE = 50000
N_LAYERS = 4
NORM_EPS = 1e-5


def scaled_normal(key_in, shape, fan_in, spread=1.0):
    return (jax.random.normal(key_in, shape, jnp.float32) * (spread * fan_in ** -0.5)).astype(jnp.bfloat16)


def draw_lengths(len_key):
    key_lo, key_hi = jax.random.split(len_key)
    lengths = jax.random.randint(key_lo, (N_ROWS,), WINDOW + 1, SEQ_LEN, jnp.int32)
    order = jax.random.permutation(key_hi, N_ROWS)
    lengths = lengths.at[order[0]].set(SEQ_LEN - 1)
    return lengths.at[order[1]].set(WINDOW + 1)


def setup_inputs(seed: int = 0, part: int = 0) -> dict:
    base_key = jax.random.key(seed)
    part_key = jax.random.fold_in(base_key, part)
    part_keys = jax.random.split(part_key, 3)
    cache_shape = (N_LAYERS, N_ROWS, KV_HEADS, SEQ_LEN, HEAD_DIM)
    k_cache = (2.5 * jax.random.normal(part_keys[0], cache_shape, jnp.float32)).astype(jnp.bfloat16)
    v_cache = jax.random.normal(part_keys[1], cache_shape, jnp.float32).astype(jnp.bfloat16)
    hidden = jax.random.normal(part_keys[2], (N_ROWS, MODEL_DIM), jnp.float32).astype(jnp.bfloat16)
    lengths = draw_lengths(jax.random.fold_in(part_key, 3))
    shared = jax.random.split(jax.random.fold_in(base_key, 1000), 8)
    q_width = N_HEADS * HEAD_DIM
    kv_width = KV_HEADS * HEAD_DIM
    ln_gain = jax.random.uniform(shared[0], (N_LAYERS, MODEL_DIM), jnp.float32, 0.5, 1.5).astype(jnp.bfloat16)
    return {
        "k_cache": k_cache,
        "v_cache": v_cache,
        "lengths": lengths,
        "hidden": hidden,
        "ln_gain": ln_gain,
        "w_query": scaled_normal(shared[1], (N_LAYERS, MODEL_DIM, q_width), MODEL_DIM),
        "w_key": scaled_normal(shared[2], (N_LAYERS, MODEL_DIM, kv_width), MODEL_DIM, 8.0),
        "w_value": scaled_normal(shared[3], (N_LAYERS, MODEL_DIM, kv_width), MODEL_DIM, 2.0),
        "w_out": scaled_normal(shared[4], (N_LAYERS, q_width, MODEL_DIM), q_width),
        "w_gate": scaled_normal(shared[5], (N_LAYERS, MODEL_DIM, FFN_DIM), MODEL_DIM),
        "w_up": scaled_normal(shared[6], (N_LAYERS, MODEL_DIM, FFN_DIM), MODEL_DIM),
        "w_down": scaled_normal(shared[7], (N_LAYERS, FFN_DIM, MODEL_DIM), FFN_DIM),
    }


def layer_norm(rows_in, gain):
    rows32 = rows_in.astype(jnp.float32)
    centered = rows32 - rows32.mean(axis=-1, keepdims=True)
    variance = (centered * centered).mean(axis=-1, keepdims=True)
    scaled = centered * lax.rsqrt(variance + NORM_EPS)
    return (scaled * gain.astype(jnp.float32)).astype(jnp.bfloat16)


def rotary(proj, positions, n_groups):
    half_dim = HEAD_DIM // 2
    inv_freq = 1.0 / (ROPE_BASE ** (jnp.arange(half_dim, dtype=jnp.float32) * 2.0 / HEAD_DIM))
    angles = positions.astype(jnp.float32)[:, None] * inv_freq[None, :]
    cosine = jnp.cos(angles)[:, None, :]
    sine = jnp.sin(angles)[:, None, :]
    heads = proj.reshape(proj.shape[0], n_groups, HEAD_DIM)
    first = heads[..., :half_dim]
    second = heads[..., half_dim:]
    turned = jnp.concatenate([first * cosine - second * sine, second * cosine + first * sine], axis=-1)
    return turned.reshape(proj.shape)


def attend(query, keys, values, key_valid):
    group_size = N_HEADS // KV_HEADS

    def one_row(row):
        q_row, k_row, v_row, ok_row = row
        grouped = q_row.reshape(KV_HEADS, group_size, HEAD_DIM).astype(jnp.float32)
        scores = jnp.einsum("kgd,ksd->kgs", grouped, k_row.astype(jnp.float32)) * HEAD_DIM ** -0.5
        scores = jnp.where(ok_row[None, None, :], scores, -1e30)
        weights = jax.nn.softmax(scores, axis=-1).astype(jnp.bfloat16)
        mixed = jnp.einsum("kgs,ksd->kgd", weights.astype(jnp.float32), v_row.astype(jnp.float32))
        return mixed.astype(jnp.bfloat16).reshape(N_HEADS * HEAD_DIM)

    return lax.map(one_row, (query, keys, values, key_valid))


def reference(k_cache, v_cache, lengths, hidden, ln_gain, w_query, w_key, w_value, w_out, w_gate, w_up, w_down):
    slot_ids = jnp.arange(WINDOW, dtype=jnp.int32)
    slot_pos = lengths[:, None] - (lengths[:, None] - slot_ids[None, :]) % WINDOW
    seq_ids = jnp.arange(SEQ_LEN, dtype=jnp.int32)
    window_valid = jnp.ones((N_ROWS, WINDOW), dtype=jnp.bool_)
    global_valid = seq_ids[None, :] <= lengths[:, None]
    before_new = (seq_ids[None, :] < lengths[:, None])[:, None, :, None]
    at_new = (seq_ids[None, :] == lengths[:, None])[:, None, :, None]
    slot_new = (slot_pos == lengths[:, None])[:, None, :, None]
    slot_index = slot_pos[:, None, :, None]
    residual = hidden
    windows_k = []
    windows_v = []
    for layer in range(N_LAYERS):
        sliding = layer < N_LAYERS - 1
        normed = layer_norm(residual, ln_gain[layer])
        query = jnp.dot(normed, w_query[layer], preferred_element_type=jnp.float32)
        key_new = jnp.dot(normed, w_key[layer], preferred_element_type=jnp.float32)
        value_new = jnp.dot(normed, w_value[layer], preferred_element_type=jnp.float32)
        if sliding:
            query = rotary(query, lengths, N_HEADS)
            key_new = rotary(key_new, lengths, KV_HEADS)
        query = query.astype(jnp.bfloat16).reshape(N_ROWS, N_HEADS, HEAD_DIM)
        key_new = key_new.astype(jnp.bfloat16).reshape(N_ROWS, KV_HEADS, 1, HEAD_DIM)
        value_new = value_new.astype(jnp.bfloat16).reshape(N_ROWS, KV_HEADS, 1, HEAD_DIM)
        if sliding:
            keys = jnp.where(slot_new, key_new, jnp.take_along_axis(k_cache[layer], slot_index, axis=2))
            values = jnp.where(slot_new, value_new, jnp.take_along_axis(v_cache[layer], slot_index, axis=2))
            windows_k.append(keys)
            windows_v.append(values)
            key_valid = window_valid
        else:
            keys = jnp.where(at_new, key_new, jnp.where(before_new, k_cache[layer], 0))
            values = jnp.where(at_new, value_new, jnp.where(before_new, v_cache[layer], 0))
            key_valid = global_valid
        mixed = attend(query, keys, values, key_valid)
        attn_out = jnp.dot(mixed, w_out[layer], preferred_element_type=jnp.float32)
        gate_proj = jnp.dot(normed, w_gate[layer], preferred_element_type=jnp.float32)
        up_proj = jnp.dot(normed, w_up[layer], preferred_element_type=jnp.float32)
        activated = (jax.nn.silu(gate_proj) * up_proj).astype(jnp.bfloat16)
        mlp_out = jnp.dot(activated, w_down[layer], preferred_element_type=jnp.float32)
        residual = (residual.astype(jnp.float32) + attn_out + mlp_out).astype(jnp.bfloat16)
    return residual, jnp.stack(windows_k), jnp.stack(windows_v), keys, values
```

```python
import functools

import jax
import jax.numpy as jnp
import numpy as np
from jax import lax
from jax.experimental import pallas as pl
from jax.experimental.pallas import tpu as pltpu
from jax.sharding import PartitionSpec as P

WINDOW = 4096
ROPE_BASE = 50000
NORM_EPS = 1e-5
LANES = 128
SUBLANES = 8
TILE = 256
F32 = jnp.float32
BF16 = jnp.bfloat16
MESH = pl.DeviceIdType.MESH


def contract_lanes(left, right):
    return lax.dot_general(left, right, (((1,), (1,)), ((), ())), preferred_element_type=F32)


def row_of(values, index):
    rows = lax.broadcasted_iota(jnp.int32, values.shape, 0)
    return jnp.where(rows == index, values, jnp.zeros_like(values))


def decode_kernel(n_sp, n_tp, len_ref, hid_ref, gain_ref, freq_row_ref, freq_col_ref, k_ref, v_ref, wq_ref, wk_ref, wv_ref, wo_ref, wg_ref, wu_ref, wd_ref,
                  hid_out, win_k_out, win_v_out, glob_k_out, glob_v_out,
                  stage, wq, wk, wv, wo, wg, wu, wd, win, glob, normed, query, act, total, sums,
                  send_sem, recv_sem, own_sem, weight_sem, out_sem, sum_send_sem, sum_recv_sem):
    n_layers = wq_ref.shape[0]
    piece = k_ref.shape[-1]
    head_dim = k_ref.shape[-2]
    q_width = wq_ref.shape[-1]
    ffn = wg_ref.shape[-1]
    dim = wq_ref.shape[1]
    n_heads = q_width // head_dim
    half = head_dim // 2
    blocks = dim // LANES
    n_low = WINDOW // piece
    me = lax.axis_index("sp")
    my_tp = lax.axis_index("tp")

    weight_pairs = ((wq_ref, wq), (wk_ref, wk), (wv_ref, wv), (wg_ref, wg), (wu_ref, wu), (wd_ref, wd), (wo_ref, wo))

    def weight_copies(layer):
        slot = layer % 2
        return [pltpu.make_async_copy(src.at[layer], dst.at[slot], weight_sem.at[slot, i]) for i, (src, dst) in enumerate(weight_pairs)]

    for copy in weight_copies(0):
        copy.start()

    barrier = pltpu.get_barrier_semaphore()
    for step in range(1, n_sp):
        pl.semaphore_signal(barrier, inc=1, device_id={"sp": lax.rem(me + step, n_sp)}, device_id_type=MESH)
    for step in range(1, n_tp):
        pl.semaphore_signal(barrier, inc=1, device_id={"tp": lax.rem(my_tp + step, n_tp)}, device_id_type=MESH)
    pl.semaphore_wait(barrier, n_sp + n_tp - 2)

    def sends(layer, kv):
        src = k_ref if kv == 0 else v_ref
        found = []
        for step in range(1, n_sp):
            dst = lax.rem(me + step, n_sp)
            found.append(pltpu.make_async_remote_copy(
                src_ref=src.at[layer, dst], dst_ref=stage.at[layer, kv, me],
                send_sem=send_sem.at[layer, kv, step], recv_sem=recv_sem.at[layer, kv, step],
                device_id={"sp": dst}, device_id_type=MESH))
        return found

    def own_copy(layer, kv):
        src = k_ref if kv == 0 else v_ref
        return pltpu.make_async_copy(src.at[layer, me], stage.at[layer, kv, me], own_sem.at[layer, kv])

    for layer in range(n_layers):
        for kv in range(2):
            for copy in sends(layer, kv):
                copy.start()
            own_copy(layer, kv).start()
    for copy in weight_copies(1):
        copy.start()

    def arrived(layer, kv):
        own_copy(layer, kv).wait()
        for copy in sends(layer, kv):
            copy.wait_recv()

    my_len = len_ref[me]
    last_slot = my_len - WINDOW
    angle_row = my_len.astype(F32) * freq_row_ref[...]
    cos_row = jnp.cos(angle_row)
    sin_row = jnp.sin(angle_row)
    angle_col = my_len.astype(F32) * freq_col_ref[...]
    cos_col = jnp.cos(angle_col)
    sin_col = jnp.sin(angle_col)
    lane_q = lax.broadcasted_iota(jnp.int32, (SUBLANES, q_width), 1)
    row_q = lax.broadcasted_iota(jnp.int32, (SUBLANES, q_width), 0)
    first_half = lax.rem(lane_q, head_dim) < half
    own_head = lax.div(lane_q, head_dim) == row_q

    residual = jnp.concatenate([hid_ref[0:1, b * LANES:(b + 1) * LANES] for b in range(blocks)], axis=0)
    out_copies = []

    def attention_query(layer, sliding):
        q = query[...]
        if sliding:
            partner = jnp.where(first_half, pltpu.roll(q, q_width - half, 1), pltpu.roll(q, half, 1))
            q = q * cos_row + jnp.where(first_half, -partner, partner) * sin_row
        q = jnp.where(own_head, q, 0.0)
        q = functools.reduce(lambda a, b: a + b, [q[:, b * LANES:(b + 1) * LANES] for b in range(q_width // LANES)])
        return (q[:, :head_dim] + q[:, head_dim:2 * head_dim]).astype(BF16)

    for layer in range(n_layers):
        sliding = layer < n_layers - 1
        slot = layer % 2
        res32 = residual.astype(F32)
        mean = jnp.sum(jnp.sum(res32, axis=1, keepdims=True), axis=0, keepdims=True) / dim
        centered = res32 - mean
        variance = jnp.sum(jnp.sum(centered * centered, axis=1, keepdims=True), axis=0, keepdims=True) / dim
        scaled = centered * lax.rsqrt(variance + NORM_EPS)
        for b in range(blocks):
            cols = slice(b * LANES, (b + 1) * LANES)
            line = scaled[b:b + 1, :] * gain_ref[layer:layer + 1, cols].astype(F32)
            normed[:, cols] = jnp.broadcast_to(line, (SUBLANES, LANES)).astype(BF16)
        waits = weight_copies(layer)
        waits[0].wait()

        @pl.loop(0, q_width // TILE)
        def _(n):
            cols = pl.ds(pl.multiple_of(n * TILE, TILE), TILE)
            query[:, cols] = jnp.dot(normed[...], wq[slot, :, cols], preferred_element_type=F32)

        q_heads = attention_query(layer, sliding)
        waits[1].wait()
        k_col = contract_lanes(wk[slot], normed[...])
        if sliding:
            first, second = k_col[:half], k_col[half:]
            k_col = jnp.concatenate([first * cos_col[:half] - second * sin_col[:half], second * cos_col[half:] + first * sin_col[half:]], axis=0)
        waits[2].wait()
        v_col = contract_lanes(wv[slot], normed[...])
        columns = (k_col[:, 0:1].astype(BF16), v_col[:, 0:1].astype(BF16))
        waits[3].wait()
        waits[4].wait()

        def gate_up(cols):
            gate = jnp.dot(normed[...], wg[slot, :, cols], preferred_element_type=F32)
            up = jnp.dot(normed[...], wu[slot, :, cols], preferred_element_type=F32)
            act[:, cols] = (gate * (1.0 / (1.0 + jnp.exp(-gate))) * up).astype(BF16)

        @pl.loop(0, ffn // TILE)
        def _(n):
            gate_up(pl.ds(pl.multiple_of(n * TILE, TILE), TILE))

        if ffn % TILE:
            gate_up(slice(ffn // TILE * TILE, ffn))
        waits[5].wait()

        @pl.loop(0, dim // TILE)
        def _(n):
            cols = pl.ds(pl.multiple_of(n * TILE, TILE), TILE)
            total[:, cols] = row_of(jnp.dot(act[...], wd[slot, :, cols], preferred_element_type=F32), 0)

        def build(kv):
            arrived(layer, kv)
            new = jnp.broadcast_to(columns[kv], (head_dim, piece))
            parts = n_low if sliding else n_sp
            for part in range(parts):
                at = slice(part * piece, (part + 1) * piece)
                ids = part * piece + lax.broadcasted_iota(jnp.int32, (head_dim, piece), 1)
                if sliding:
                    value = jnp.where(ids < last_slot, stage[layer, kv, part + n_low], stage[layer, kv, part])
                    value = jnp.where(ids == last_slot, new, value)
                    win[slot, kv, :, at] = value
                else:
                    value = jnp.where(ids < my_len, stage[layer, kv, part], jnp.zeros_like(new))
                    value = jnp.where(ids == my_len, new, value)
                    glob[kv, :, at] = value
            if sliding:
                target = win_k_out if kv == 0 else win_v_out
                copy = pltpu.make_async_copy(win.at[slot, kv], target.at[layer], out_sem.at[layer, kv])
            else:
                target = glob_k_out if kv == 0 else glob_v_out
                copy = pltpu.make_async_copy(glob.at[kv], target, out_sem.at[layer, kv])
            copy.start()
            out_copies.append(copy)

        if layer >= 2 and sliding:
            for copy in out_copies[2 * (layer - 2):2 * (layer - 1)]:
                copy.wait()
        build(0)
        keys = win[slot, 0] if sliding else glob[0]
        scores = jnp.dot(q_heads, keys, preferred_element_type=F32) * head_dim ** -0.5
        if not sliding:
            ids = lax.broadcasted_iota(jnp.int32, scores.shape, 1)
            scores = jnp.where(ids <= my_len, scores, -1e30)
        top = jnp.max(scores, axis=1, keepdims=True)
        weights = jnp.exp(scores - top)
        weights = (weights * (1.0 / jnp.sum(weights, axis=1, keepdims=True))).astype(BF16)
        build(1)
        values = win[slot, 1] if sliding else glob[1]
        mixed = contract_lanes(weights, values)
        mixed = jnp.concatenate([mixed] * n_heads, axis=1)
        mixed = jnp.where(own_head, mixed, 0.0).astype(BF16)
        waits[6].wait()

        @pl.loop(0, dim // TILE)
        def _(n):
            cols = pl.ds(pl.multiple_of(n * TILE, TILE), TILE)
            total[:, cols] += jnp.dot(mixed, wo[slot, :, cols], preferred_element_type=F32)

        if layer + 2 < n_layers:
            for copy in weight_copies(layer + 2):
                copy.start()
        for b in range(blocks):
            sums[layer, my_tp, b:b + 1, :] = jnp.sum(total[:, b * LANES:(b + 1) * LANES], axis=0, keepdims=True)
        reduces = [pltpu.make_async_remote_copy(
            src_ref=sums.at[layer, my_tp], dst_ref=sums.at[layer, my_tp],
            send_sem=sum_send_sem.at[layer, step], recv_sem=sum_recv_sem.at[layer, step],
            device_id={"tp": lax.rem(my_tp + step, n_tp)}, device_id_type=MESH) for step in range(1, n_tp)]
        for copy in reduces:
            copy.start()
        for copy in reduces:
            copy.wait_recv()
        summed = res32
        for other in range(n_tp):
            summed = summed + sums[layer, other]
        residual = summed.astype(BF16)
        for copy in reduces:
            copy.wait_send()

    for b in range(blocks):
        hid_out[0:1, b * LANES:(b + 1) * LANES] = residual[b:b + 1, :]
    waited = 2 * max(0, n_layers - 1 - 2)
    for copy in out_copies[waited:]:
        copy.wait()
    for layer in range(n_layers):
        for kv in range(2):
            for copy in sends(layer, kv):
                copy.wait_send()


def solution(mesh):
    cache_spec = P(None, "dp", "tp", "sp", None)
    row_spec = P(("dp", "sp"), None)
    col_spec = P(None, None, "tp")
    inner_spec = P(None, "tp", None)
    window_spec = P(None, ("dp", "sp"), "tp", None, None)
    global_spec = P(("dp", "sp"), "tp", None, None)
    in_specs = (cache_spec, cache_spec, P("dp"), row_spec, P(None, None), col_spec, col_spec, col_spec, inner_spec, col_spec, col_spec, inner_spec)
    out_specs = (row_spec, window_spec, window_spec, global_spec, global_spec)
    n_sp, n_tp = mesh.shape["sp"], mesh.shape["tp"]

    def device_step(k_cache, v_cache, lengths, hidden, ln_gain, w_query, w_key, w_value, w_out, w_gate, w_up, w_down):
        n_layers, dim, q_width = w_query.shape
        n_rows, _, piece, head_dim = k_cache.shape[1:]
        ffn = w_gate.shape[-1]
        seq_len = piece * n_sp
        cache_k = jnp.swapaxes(k_cache, 3, 4).reshape(n_layers, n_rows, head_dim, piece)
        cache_v = jnp.swapaxes(v_cache, 3, 4).reshape(n_layers, n_rows, head_dim, piece)
        half = head_dim // 2
        freq = np.float32(1.0) / np.power(np.float32(ROPE_BASE), np.arange(half, dtype=np.float32) * np.float32(2.0) / np.float32(head_dim))
        freq_row = np.tile(freq.astype(np.float32), (SUBLANES, q_width // half))
        freq_col = np.tile(freq.astype(np.float32)[:, None], (2, SUBLANES))
        vmem = pl.BlockSpec(memory_space=pltpu.VMEM)
        hbm = pl.BlockSpec(memory_space=pl.ANY)
        hid, win_k, win_v, glob_k, glob_v = pl.pallas_call(
            functools.partial(decode_kernel, n_sp, n_tp),
            out_shape=(
                jax.ShapeDtypeStruct((1, dim), BF16),
                jax.ShapeDtypeStruct((n_layers - 1, head_dim, WINDOW), BF16),
                jax.ShapeDtypeStruct((n_layers - 1, head_dim, WINDOW), BF16),
                jax.ShapeDtypeStruct((head_dim, seq_len), BF16),
                jax.ShapeDtypeStruct((head_dim, seq_len), BF16),
            ),
            in_specs=[pl.BlockSpec(memory_space=pltpu.SMEM)] + [vmem] * 4 + [hbm] * 9,
            out_specs=(vmem, hbm, hbm, hbm, hbm),
            scratch_shapes=[
                pltpu.VMEM((n_layers, 2, n_sp, head_dim, piece), BF16),
                pltpu.VMEM((2, dim, q_width), BF16),
                pltpu.VMEM((2, head_dim, dim), BF16),
                pltpu.VMEM((2, head_dim, dim), BF16),
                pltpu.VMEM((2, q_width, dim), BF16),
                pltpu.VMEM((2, dim, ffn), BF16),
                pltpu.VMEM((2, dim, ffn), BF16),
                pltpu.VMEM((2, ffn, dim), BF16),
                pltpu.VMEM((2, 2, head_dim, WINDOW), BF16),
                pltpu.VMEM((2, head_dim, seq_len), BF16),
                pltpu.VMEM((SUBLANES, dim), BF16),
                pltpu.VMEM((SUBLANES, q_width), F32),
                pltpu.VMEM((SUBLANES, ffn), BF16),
                pltpu.VMEM((SUBLANES, dim), F32),
                pltpu.VMEM((n_layers, n_tp, dim // LANES, LANES), F32),
                pltpu.SemaphoreType.DMA((n_layers, 2, n_sp)),
                pltpu.SemaphoreType.DMA((n_layers, 2, n_sp)),
                pltpu.SemaphoreType.DMA((n_layers, 2)),
                pltpu.SemaphoreType.DMA((2, 7)),
                pltpu.SemaphoreType.DMA((n_layers, 2)),
                pltpu.SemaphoreType.DMA((n_layers, n_tp)),
                pltpu.SemaphoreType.DMA((n_layers, n_tp)),
            ],
            compiler_params=pltpu.CompilerParams(collective_id=0, has_side_effects=True, vmem_limit_bytes=60 << 20),
        )(lengths, hidden, ln_gain, freq_row, freq_col, cache_k, cache_v, w_query, jnp.swapaxes(w_key, 1, 2), jnp.swapaxes(w_value, 1, 2), w_out, w_gate, w_up, w_down)

        def back(array):
            lead = array.shape[:-2]
            return jnp.swapaxes(array.reshape(lead + (1, 1) + array.shape[-2:]), -2, -1)

        return hid, back(win_k), back(win_v), back(glob_k), back(glob_v)

    return jax.shard_map(device_step, mesh=mesh, in_specs=in_specs, out_specs=out_specs, check_vma=False)
```

```python
import functools

import jax
import jax.numpy as jnp
import numpy as np
from jax import lax
from jax.experimental import pallas as pl
from jax.experimental.pallas import tpu as pltpu
from jax.sharding import PartitionSpec as P

WINDOW = 4096
ROPE_BASE = 50000
NORM_EPS = 1e-5
LANES = 128
SUBLANES = 8
TILE = 256
CORES = 2
F32 = jnp.float32
BF16 = jnp.bfloat16
MESH = pl.DeviceIdType.MESH


def contract_lanes(left, right):
    return lax.dot_general(left, right, (((1,), (1,)), ((), ())), preferred_element_type=F32)


def write_kernel(*refs):
    count = (len(refs) - 1) // 2
    sources, targets, sem = refs[:count], refs[count:2 * count], refs[-1]
    copies = [pltpu.make_async_copy(src, dst, sem.at[i]) for i, (src, dst) in enumerate(zip(sources, targets))]
    for copy in copies:
        copy.start()
    for copy in copies:
        copy.wait()


def decode_kernel(n_sp, n_tp, len_ref, hid_ref, gain_ref, freq_row_ref, freq_col_ref, k_ref, v_ref, wq_ref, wk_ref, wv_ref, wo_ref, wg_ref, wu_ref, wd_ref,
                  hid_out, win_k_out, win_v_out, glob_k_out, glob_v_out,
                  stage, wq, wk, wv, wo, wg, wu, wd, normed, query, act, mlp, sums,
                  send_sem, recv_sem, own_sem, weight_sem, sum_send_sem, sum_recv_sem):
    n_layers = wq_ref.shape[0]
    piece = k_ref.shape[-1]
    head_dim = k_ref.shape[-2]
    q_width = wq_ref.shape[-1]
    ffn = wg_ref.shape[-1]
    dim = wq_ref.shape[1]
    n_heads = q_width // head_dim
    half = head_dim // 2
    blocks = dim // LANES
    n_low = WINDOW // piece
    me = lax.axis_index("sp")
    my_tp = lax.axis_index("tp")

    weight_pairs = ((wq_ref, wq), (wk_ref, wk), (wv_ref, wv), (wg_ref, wg), (wu_ref, wu), (wd_ref, wd), (wo_ref, wo))

    def weight_copies(layer):
        slot = layer % 2
        return [pltpu.make_async_copy(src.at[layer], dst.at[slot], weight_sem.at[slot, i]) for i, (src, dst) in enumerate(weight_pairs)]

    for copy in weight_copies(0):
        copy.start()

    barrier = pltpu.get_barrier_semaphore()
    for step in range(1, n_sp):
        pl.semaphore_signal(barrier, inc=1, device_id={"sp": lax.rem(me + step, n_sp)}, device_id_type=MESH)
    for step in range(1, n_tp):
        pl.semaphore_signal(barrier, inc=1, device_id={"tp": lax.rem(my_tp + step, n_tp)}, device_id_type=MESH)
    pl.semaphore_wait(barrier, n_sp + n_tp - 2)

    chips = n_sp // CORES
    chip, core = lax.div(me, CORES), lax.rem(me, CORES)
    far_first = sorted(range(1, chips), key=lambda d: -min(d, chips - d))
    chip_order = [0] + far_first
    deltas = [(dc, dk) for dc in chip_order for dk in range(CORES) if (dc, dk) != (0, 0)]

    def shifted(dc, dk):
        return lax.rem(chip + dc, chips) * CORES + lax.rem(core + dk, CORES)

    def send(layer, kv, dc, dk):
        src = k_ref if kv == 0 else v_ref
        dst = shifted(dc, dk)
        at = dc * CORES + dk
        return pltpu.make_async_remote_copy(
            src_ref=src.at[layer, dst], dst_ref=stage.at[layer, kv, me],
            send_sem=send_sem.at[layer, kv, at], recv_sem=recv_sem.at[layer, kv, at],
            device_id={"sp": dst}, device_id_type=MESH)

    def sends(layer, kv):
        return [send(layer, kv, dc, dk) for dc, dk in deltas]

    def own_copy(layer, kv):
        src = k_ref if kv == 0 else v_ref
        return pltpu.make_async_copy(src.at[layer, me], stage.at[layer, kv, me], own_sem.at[layer, kv])

    for layer in range(n_layers):
        for kv in range(2):
            for copy in sends(layer, kv):
                copy.start()
            own_copy(layer, kv).start()
    for copy in weight_copies(1):
        copy.start()

    def wait_from(layer, kv, dc, dk):
        if (dc, dk) == (0, 0):
            own_copy(layer, kv).wait()
        else:
            send(layer, kv, (chips - dc) % chips, dk).wait_recv()

    my_len = len_ref[me]
    last_slot = my_len - WINDOW
    angle_row = my_len.astype(F32) * freq_row_ref[...]
    cos_row = jnp.cos(angle_row)
    sin_row = jnp.sin(angle_row)
    angle_col = my_len.astype(F32) * freq_col_ref[...]
    cos_col = jnp.cos(angle_col)
    sin_col = jnp.sin(angle_col)
    lane_q = lax.broadcasted_iota(jnp.int32, (SUBLANES, q_width), 1)
    row_q = lax.broadcasted_iota(jnp.int32, (SUBLANES, q_width), 0)
    first_half = lax.rem(lane_q, head_dim) < half
    own_head = lax.div(lane_q, head_dim) == row_q

    residual = jnp.concatenate([hid_ref[0:1, b * LANES:(b + 1) * LANES] for b in range(blocks)], axis=0)

    def attention_query(layer, sliding):
        q = query[...]
        if sliding:
            partner = jnp.where(first_half, pltpu.roll(q, q_width - half, 1), pltpu.roll(q, half, 1))
            q = q * cos_row + jnp.where(first_half, -partner, partner) * sin_row
        q = jnp.where(own_head, q, 0.0)
        q = functools.reduce(lambda a, b: a + b, [q[:, b * LANES:(b + 1) * LANES] for b in range(q_width // LANES)])
        return (q[:, :head_dim] + q[:, head_dim:2 * head_dim]).astype(BF16)

    for layer in range(n_layers):
        sliding = layer < n_layers - 1
        slot = layer % 2
        res32 = residual.astype(F32)
        mean = jnp.sum(jnp.sum(res32, axis=1, keepdims=True), axis=0, keepdims=True) / dim
        centered = res32 - mean
        variance = jnp.sum(jnp.sum(centered * centered, axis=1, keepdims=True), axis=0, keepdims=True) / dim
        scaled = centered * lax.rsqrt(variance + NORM_EPS)
        for b in range(blocks):
            cols = slice(b * LANES, (b + 1) * LANES)
            line = scaled[b:b + 1, :] * gain_ref[layer:layer + 1, cols].astype(F32)
            normed[:, cols] = jnp.broadcast_to(line, (SUBLANES, LANES)).astype(BF16)
        waits = weight_copies(layer)
        waits[0].wait()

        @pl.loop(0, q_width // TILE)
        def _(n):
            cols = pl.ds(pl.multiple_of(n * TILE, TILE), TILE)
            query[:, cols] = jnp.dot(normed[...], wq[slot, :, cols], preferred_element_type=F32)

        q_heads = attention_query(layer, sliding)
        waits[1].wait()
        k_col = contract_lanes(wk[slot], normed[...])
        if sliding:
            first, second = k_col[:half], k_col[half:]
            k_col = jnp.concatenate([first * cos_col[:half] - second * sin_col[:half], second * cos_col[half:] + first * sin_col[half:]], axis=0)
        waits[2].wait()
        v_col = contract_lanes(wv[slot], normed[...])
        columns = (k_col[:, 0:1].astype(BF16), v_col[:, 0:1].astype(BF16))
        waits[3].wait()
        waits[4].wait()

        def gate_up(cols):
            gate = jnp.dot(normed[...], wg[slot, :, cols], preferred_element_type=F32)
            up = jnp.dot(normed[...], wu[slot, :, cols], preferred_element_type=F32)
            act[:, cols] = (gate * (1.0 / (1.0 + jnp.exp(-gate))) * up).astype(BF16)

        @pl.loop(0, ffn // TILE)
        def _(n):
            gate_up(pl.ds(pl.multiple_of(n * TILE, TILE), TILE))

        if ffn % TILE:
            gate_up(slice(ffn // TILE * TILE, ffn))
        waits[5].wait()

        @pl.loop(0, dim // TILE)
        def _(n):
            cols = pl.ds(pl.multiple_of(n * TILE, TILE), TILE)
            down = jnp.dot(act[...], wd[slot, :, cols], preferred_element_type=F32)
            mlp[:, cols] = down[0:1]

        def pieces(kv):
            new = jnp.broadcast_to(columns[kv], (head_dim, piece))
            lanes = lax.broadcasted_iota(jnp.int32, (head_dim, piece), 1)
            if sliding:
                target = (win_k_out if kv == 0 else win_v_out).at[layer]
                half_chips = chips // 2
                for dc in sorted(range(half_chips)):
                    for dk in range(CORES):
                        wait_from(layer, kv, dc, dk)
                        wait_from(layer, kv, dc + half_chips, dk)
                        part = lax.rem(shifted(dc, dk), n_low)
                        ids = part * piece + lanes
                        value = jnp.where(ids < last_slot, stage[layer, kv, part + n_low], stage[layer, kv, part])
                        value = jnp.where(ids == last_slot, new, value)
                        target[:, pl.ds(pl.multiple_of(part * piece, piece), piece)] = value
                        yield part, value
            else:
                target = glob_k_out if kv == 0 else glob_v_out
                for dc in chip_order:
                    for dk in range(CORES):
                        wait_from(layer, kv, dc, dk)
                        part = shifted(dc, dk)
                        ids = part * piece + lanes
                        value = jnp.where(ids < my_len, stage[layer, kv, part], jnp.zeros_like(new))
                        value = jnp.where(ids == my_len, new, value)
                        target[:, pl.ds(pl.multiple_of(part * piece, piece), piece)] = value
                        yield part, value

        scores = []
        for part, keys in pieces(0):
            score = jnp.dot(q_heads, keys, preferred_element_type=F32) * head_dim ** -0.5
            if not sliding:
                ids = part * piece + lax.broadcasted_iota(jnp.int32, score.shape, 1)
                score = jnp.where(ids <= my_len, score, -1e30)
            scores.append(score)
        top = functools.reduce(jnp.maximum, [jnp.max(score, axis=1, keepdims=True) for score in scores])
        scores = [jnp.exp(score - top) for score in scores]
        share = 1.0 / functools.reduce(jnp.add, [jnp.sum(score, axis=1, keepdims=True) for score in scores])
        weights = [(score * share).astype(BF16) for score in scores]
        mixed = functools.reduce(jnp.add, [contract_lanes(weight, values) for weight, (part, values) in zip(weights, pieces(1))])
        mixed = jnp.where(own_head, jnp.concatenate([mixed] * n_heads, axis=1), 0.0)
        mixed = jnp.broadcast_to(jnp.sum(mixed, axis=0, keepdims=True), mixed.shape).astype(BF16)
        waits[6].wait()
        for n in range(dim // TILE):
            attn = jnp.dot(mixed, wo[slot, :, n * TILE:(n + 1) * TILE], preferred_element_type=F32)
            for b in range(n * TILE // LANES, (n + 1) * TILE // LANES):
                inner = slice(b * LANES - n * TILE, (b + 1) * LANES - n * TILE)
                sums[layer, my_tp, b:b + 1, :] = attn[0:1, inner] + mlp[:, b * LANES:(b + 1) * LANES]
        if layer + 2 < n_layers:
            for copy in weight_copies(layer + 2):
                copy.start()
        reduces = [pltpu.make_async_remote_copy(
            src_ref=sums.at[layer, my_tp], dst_ref=sums.at[layer, my_tp],
            send_sem=sum_send_sem.at[layer, step], recv_sem=sum_recv_sem.at[layer, step],
            device_id={"tp": lax.rem(my_tp + step, n_tp)}, device_id_type=MESH) for step in range(1, n_tp)]
        for copy in reduces:
            copy.start()
        for copy in reduces:
            copy.wait_recv()
        summed = res32
        for other in range(n_tp):
            summed = summed + sums[layer, other]
        residual = summed.astype(BF16)
        for copy in reduces:
            copy.wait_send()

    for b in range(blocks):
        hid_out[0:1, b * LANES:(b + 1) * LANES] = residual[b:b + 1, :]
    for layer in range(n_layers):
        for kv in range(2):
            for copy in sends(layer, kv):
                copy.wait_send()


def solution(mesh):
    cache_spec = P(None, "dp", "tp", "sp", None)
    row_spec = P(("dp", "sp"), None)
    col_spec = P(None, None, "tp")
    inner_spec = P(None, "tp", None)
    window_spec = P(None, ("dp", "sp"), "tp", None, None)
    global_spec = P(("dp", "sp"), "tp", None, None)
    in_specs = (cache_spec, cache_spec, P("dp"), row_spec, P(None, None), col_spec, col_spec, col_spec, inner_spec, col_spec, col_spec, inner_spec)
    out_specs = (row_spec, window_spec, window_spec, global_spec, global_spec)
    n_sp, n_tp = mesh.shape["sp"], mesh.shape["tp"]

    def device_step(k_cache, v_cache, lengths, hidden, ln_gain, w_query, w_key, w_value, w_out, w_gate, w_up, w_down):
        n_layers, dim, q_width = w_query.shape
        n_rows, _, piece, head_dim = k_cache.shape[1:]
        ffn = w_gate.shape[-1]
        seq_len = piece * n_sp
        cache_k = jnp.swapaxes(k_cache, 3, 4).reshape(n_layers, n_rows, head_dim, piece)
        cache_v = jnp.swapaxes(v_cache, 3, 4).reshape(n_layers, n_rows, head_dim, piece)
        half = head_dim // 2
        freq = np.float32(1.0) / np.power(np.float32(ROPE_BASE), np.arange(half, dtype=np.float32) * np.float32(2.0) / np.float32(head_dim))
        freq_row = np.tile(freq.astype(np.float32), (SUBLANES, q_width // half))
        freq_col = np.tile(freq.astype(np.float32)[:, None], (2, SUBLANES))
        vmem = pl.BlockSpec(memory_space=pltpu.VMEM)
        hbm = pl.BlockSpec(memory_space=pl.ANY)
        shapes = [(1, dim)] + [(n_layers - 1, head_dim, WINDOW)] * 2 + [(head_dim, seq_len)] * 2
        results = pl.pallas_call(
            functools.partial(decode_kernel, n_sp, n_tp),
            out_shape=[pltpu.VMEM(shape, BF16) for shape in shapes],
            in_specs=[pl.BlockSpec(memory_space=pltpu.SMEM)] + [vmem] * 4 + [hbm] * 9,
            out_specs=[vmem] * len(shapes),
            scratch_shapes=[
                pltpu.VMEM((n_layers, 2, n_sp, head_dim, piece), BF16),
                pltpu.VMEM((2, dim, q_width), BF16),
                pltpu.VMEM((2, head_dim, dim), BF16),
                pltpu.VMEM((2, head_dim, dim), BF16),
                pltpu.VMEM((2, q_width, dim), BF16),
                pltpu.VMEM((2, dim, ffn), BF16),
                pltpu.VMEM((2, dim, ffn), BF16),
                pltpu.VMEM((2, ffn, dim), BF16),
                pltpu.VMEM((SUBLANES, dim), BF16),
                pltpu.VMEM((SUBLANES, q_width), F32),
                pltpu.VMEM((SUBLANES, ffn), BF16),
                pltpu.VMEM((1, dim), F32),
                pltpu.VMEM((n_layers, n_tp, dim // LANES, LANES), F32),
                pltpu.SemaphoreType.DMA((n_layers, 2, n_sp)),
                pltpu.SemaphoreType.DMA((n_layers, 2, n_sp)),
                pltpu.SemaphoreType.DMA((n_layers, 2)),
                pltpu.SemaphoreType.DMA((2, 7)),
                pltpu.SemaphoreType.DMA((n_layers, n_tp)),
                pltpu.SemaphoreType.DMA((n_layers, n_tp)),
            ],
            compiler_params=pltpu.CompilerParams(collective_id=0, has_side_effects=True, vmem_limit_bytes=53 << 20),
        )(lengths, hidden, ln_gain, freq_row, freq_col, cache_k, cache_v, w_query, jnp.swapaxes(w_key, 1, 2), jnp.swapaxes(w_value, 1, 2), w_out, w_gate, w_up, w_down)

        hid, win_k, win_v, glob_k, glob_v = pl.pallas_call(
            write_kernel,
            out_shape=[jax.ShapeDtypeStruct(shape, BF16) for shape in shapes],
            in_specs=[vmem] * len(shapes),
            out_specs=[hbm] * len(shapes),
            scratch_shapes=[pltpu.SemaphoreType.DMA((len(shapes),))],
            compiler_params=pltpu.CompilerParams(vmem_limit_bytes=1 << 20),
        )(*[pltpu.with_memory_space_constraint(result, pltpu.VMEM) for result in results])

        def back(array):
            lead = array.shape[:-2]
            return jnp.swapaxes(array.reshape(lead + (1, 1) + array.shape[-2:]), -2, -1)

        return hid, back(win_k), back(win_v), back(glob_k), back(glob_v)

    return jax.shard_map(device_step, mesh=mesh, in_specs=in_specs, out_specs=out_specs, check_vma=False)
```

```python
import functools

import jax
import jax.numpy as jnp
import numpy as np
from jax import lax
from jax.experimental import pallas as pl
from jax.experimental.pallas import tpu as pltpu
from jax.sharding import PartitionSpec as P

WINDOW = 4096
ROPE_BASE = 50000
NORM_EPS = 1e-5
LANES = 128
SUBLANES = 8
TILE = 256
CORES = 2
F32 = jnp.float32
BF16 = jnp.bfloat16
MESH = pl.DeviceIdType.MESH


def contract_lanes(left, right):
    return lax.dot_general(left, right, (((1,), (1,)), ((), ())), preferred_element_type=F32)


def write_kernel(*refs):
    count = (len(refs) - 1) // 2
    sources, targets, sem = refs[:count], refs[count:2 * count], refs[-1]
    copies = [pltpu.make_async_copy(src, dst, sem.at[i]) for i, (src, dst) in enumerate(zip(sources, targets))]
    for copy in copies:
        copy.start()
    for copy in copies:
        copy.wait()


def decode_kernel(n_sp, n_tp, len_in, hid_in, gain_in, freq_row_in, freq_col_in, k_ref, v_ref, wq_ref, wk_ref, wv_ref, wo_ref, wg_ref, wu_ref, wd_ref,
                  hid_out, win_k_out, win_v_out, glob_k_out, glob_v_out,
                  stage, wq, wk, wv, wo, wg, wu, wd, normed, query, act, mlp, sums, len_ref, hid_ref, gain_ref, freq_row_ref, freq_col_ref,
                  local, local_score, queries, stats, values_out, values_in,
                  send_sem, recv_sem, own_sem, weight_sem, small_sem, sum_send_sem, sum_recv_sem, local_sem, message_send_sem, message_recv_sem, line_sem, ready_sem):
    n_layers = wq_ref.shape[0]
    piece = k_ref.shape[-1]
    head_dim = k_ref.shape[-2]
    q_width = wq_ref.shape[-1]
    ffn = wg_ref.shape[-1]
    dim = wq_ref.shape[1]
    n_heads = q_width // head_dim
    half = head_dim // 2
    blocks = dim // LANES
    n_low = WINDOW // piece
    me = lax.axis_index("sp")
    my_tp = lax.axis_index("tp")

    weight_pairs = ((wq_ref, wq), (wk_ref, wk), (wv_ref, wv), (wg_ref, wg), (wu_ref, wu), (wd_ref, wd), (wo_ref, wo))

    def weight_copies(layer):
        slot = layer % 2
        return [pltpu.make_async_copy(src.at[layer], dst.at[slot], weight_sem.at[slot, i]) for i, (src, dst) in enumerate(weight_pairs)]

    barrier = pltpu.get_barrier_semaphore()
    for step in range(1, n_sp):
        pl.semaphore_signal(barrier, inc=1, device_id={"sp": lax.rem(me + step, n_sp)}, device_id_type=MESH)
    lead = me == 0

    @pl.when(lead)
    def _():
        for step in range(1, n_tp):
            pl.semaphore_signal(barrier, inc=1, device_id={"tp": lax.rem(my_tp + step, n_tp)}, device_id_type=MESH)
        pl.semaphore_wait(barrier, n_sp + n_tp - 2)

    @pl.when(jnp.logical_not(lead))
    def _():
        pl.semaphore_wait(barrier, n_sp - 1)

    chips = n_sp // CORES
    chip, core = lax.div(me, CORES), lax.rem(me, CORES)
    far_first = sorted(range(1, chips), key=lambda d: -min(d, chips - d))
    chip_order = [0] + far_first
    deltas = [(dc, dk) for dc in chip_order for dk in range(CORES) if (dc, dk) != (0, 0)]

    def shifted(dc, dk):
        return lax.rem(chip + dc, chips) * CORES + lax.rem(core + dk, CORES)

    def send(layer, kv, dc, dk):
        src = k_ref if kv == 0 else v_ref
        dst = shifted(dc, dk)
        at = dc * CORES + dk
        return pltpu.make_async_remote_copy(
            src_ref=src.at[layer, dst], dst_ref=stage.at[layer, kv, me],
            send_sem=send_sem.at[layer, kv, at], recv_sem=recv_sem.at[layer, kv, at],
            device_id={"sp": dst}, device_id_type=MESH)

    def sends(layer, kv):
        return [send(layer, kv, dc, dk) for dc, dk in deltas]

    def own_copy(layer, kv):
        src = k_ref if kv == 0 else v_ref
        return pltpu.make_async_copy(src.at[layer, me], stage.at[layer, kv, me], own_sem.at[layer, kv])

    def start_bulk(layer, kv):
        for copy in sends(layer, kv):
            copy.start()
        own_copy(layer, kv).start()

    bulk_order = [(layer, kv) for layer in list(range(1, n_layers)) + [0] for kv in range(2)]
    start_bulk(*bulk_order[0])
    small_pairs = ((len_in, len_ref), (hid_in, hid_ref), (gain_in, gain_ref), (freq_row_in, freq_row_ref), (freq_col_in, freq_col_ref))
    small_copies = [pltpu.make_async_copy(src, dst, small_sem.at[i]) for i, (src, dst) in enumerate(small_pairs)]
    local_copies = [pltpu.make_async_copy(src.at[0], local.at[kv], local_sem.at[kv]) for kv, src in enumerate((k_ref, v_ref))]
    first_weights = weight_copies(0)
    for copy in small_copies + first_weights[:3]:
        copy.start()

    @pl.when(lead)
    def _():
        for step in range(1, n_tp):
            pl.semaphore_signal(line_sem, inc=1, device_id={"tp": lax.rem(my_tp + step, n_tp)}, device_id_type=MESH)
        pl.semaphore_wait(line_sem, n_tp - 1)
        for step in range(1, n_sp):
            pl.semaphore_signal(ready_sem, inc=1, device_id={"sp": lax.rem(me + step, n_sp)}, device_id_type=MESH)

    for copy in small_copies:
        copy.wait()

    def messages(kind, source, target):
        found = []
        for step in range(1, n_sp):
            dst = lax.rem(me + step, n_sp)
            found.append(pltpu.make_async_remote_copy(
                src_ref=source(dst), dst_ref=target,
                send_sem=message_send_sem.at[kind, step], recv_sem=message_recv_sem.at[kind, step],
                device_id={"sp": dst}, device_id_type=MESH))
        for copy in found:
            copy.start()
        return found

    def wait_from(layer, kv, dc, dk):
        if (dc, dk) == (0, 0):
            own_copy(layer, kv).wait()
        else:
            send(layer, kv, (chips - dc) % chips, dk).wait_recv()

    my_len = len_ref[me]
    last_slot = my_len - WINDOW
    angle_row = my_len.astype(F32) * freq_row_ref[...]
    cos_row = jnp.cos(angle_row)
    sin_row = jnp.sin(angle_row)
    angle_col = my_len.astype(F32) * freq_col_ref[...]
    cos_col = jnp.cos(angle_col)
    sin_col = jnp.sin(angle_col)
    lane_q = lax.broadcasted_iota(jnp.int32, (SUBLANES, q_width), 1)
    row_q = lax.broadcasted_iota(jnp.int32, (SUBLANES, q_width), 0)
    first_half = lax.rem(lane_q, head_dim) < half
    own_head = lax.div(lane_q, head_dim) == row_q

    residual = jnp.concatenate([hid_ref[0:1, b * LANES:(b + 1) * LANES] for b in range(blocks)], axis=0)

    lane_t = lax.broadcasted_iota(jnp.int32, (SUBLANES, LANES), 1)
    all_messages = []

    def attention_query(layer, sliding):
        q = query[...]
        if sliding:
            partner = jnp.where(first_half, pltpu.roll(q, q_width - half, 1), pltpu.roll(q, half, 1))
            q = q * cos_row + jnp.where(first_half, -partner, partner) * sin_row
        q = jnp.where(own_head, q, 0.0)
        q = functools.reduce(lambda a, b: a + b, [q[:, b * LANES:(b + 1) * LANES] for b in range(q_width // LANES)])
        return (q + pltpu.roll(q, head_dim, 1)).astype(BF16)

    def pieces(layer, kv, columns):
        sliding = layer < n_layers - 1
        new = jnp.broadcast_to(columns[kv], (head_dim, piece))
        lanes = lax.broadcasted_iota(jnp.int32, (head_dim, piece), 1)
        if sliding:
            target = (win_k_out if kv == 0 else win_v_out).at[layer]
            half_chips = chips // 2
            for dc in sorted(range(half_chips)):
                for dk in range(CORES):
                    wait_from(layer, kv, dc, dk)
                    wait_from(layer, kv, dc + half_chips, dk)
                    part = lax.rem(shifted(dc, dk), n_low)
                    ids = part * piece + lanes
                    value = jnp.where(ids < last_slot, stage[layer, kv, part + n_low], stage[layer, kv, part])
                    value = jnp.where(ids == last_slot, new, value)
                    target[:, pl.ds(pl.multiple_of(part * piece, piece), piece)] = value
                    yield part, value
        else:
            target = glob_k_out if kv == 0 else glob_v_out
            for dc in chip_order:
                for dk in range(CORES):
                    wait_from(layer, kv, dc, dk)
                    part = shifted(dc, dk)
                    ids = part * piece + lanes
                    value = jnp.where(ids < my_len, stage[layer, kv, part], jnp.zeros_like(new))
                    value = jnp.where(ids == my_len, new, value)
                    target[:, pl.ds(pl.multiple_of(part * piece, piece), piece)] = value
                    yield part, value

    def spread_attention(q_heads, k_new, v_row, sent):
        for copy in sent:
            copy.wait_recv()
        local_copies[0].wait()
        positions = me * piece + lax.broadcasted_iota(jnp.int32, (SUBLANES, piece), 1)
        new_score = jnp.dot(q_heads, jnp.broadcast_to(k_new, (head_dim, LANES)), preferred_element_type=F32) * head_dim ** -0.5
        tops = jnp.zeros((SUBLANES, LANES), F32)
        norms = jnp.zeros((SUBLANES, LANES), F32)
        for row in range(n_sp):
            score = jnp.dot(queries[row][:, :head_dim].astype(BF16), local[0, row], preferred_element_type=F32) * head_dim ** -0.5
            valid = (positions > len_ref[row] - WINDOW) & (positions < len_ref[row])
            score = jnp.where(valid, score, -1e30)
            local_score[row] = score
            top = jnp.max(score, axis=1, keepdims=True)
            norm = jnp.sum(jnp.exp(score - top), axis=1, keepdims=True)
            tops = jnp.where(lane_t == row, top, tops)
            norms = jnp.where(lane_t == row, norm, norms)
        mine = lane_t == me
        raised = jnp.where(mine, jnp.maximum(tops, new_score), tops)
        norms = jnp.where(mine, norms * jnp.exp(tops - raised) + jnp.exp(jnp.where(mine, new_score - raised, 0.0)), norms)
        stats[me, 0] = raised
        stats[me, 1] = norms
        sent = messages(1, lambda dst: stats.at[me], stats.at[me])
        all_messages.extend(sent)
        start_bulk(*bulk_order[2])
        for copy in weight_copies(1):
            copy.start()
        for copy in sent:
            copy.wait_recv()
        local_copies[1].wait()
        top = functools.reduce(jnp.maximum, [stats[src, 0] for src in range(n_sp)])
        norm = functools.reduce(jnp.add, [stats[src, 1] * jnp.exp(stats[src, 0] - top) for src in range(n_sp)])
        share = 1.0 / jnp.where(lane_t < n_sp, norm, 1.0)
        for row in range(n_sp):
            weight = (jnp.exp(local_score[row] - top[:, row:row + 1]) * share[:, row:row + 1]).astype(BF16)
            partial = contract_lanes(weight, local[1, row])
            values_out[row] = jnp.concatenate([partial, partial], axis=1)
        sent = messages(2, lambda dst: values_out.at[dst], values_in.at[me])
        all_messages.extend(sent)
        for group in bulk_order[3:]:
            start_bulk(*group)
        my_top = jnp.sum(jnp.where(mine, top, 0.0), axis=1, keepdims=True)
        my_share = jnp.sum(jnp.where(mine, share, 0.0), axis=1, keepdims=True)
        new_weight = (jnp.exp(new_score[:, 0:1] - my_top) * my_share).astype(BF16).astype(F32)
        mixed = new_weight * v_row + values_out[me][:, :head_dim]
        for copy in sent:
            copy.wait_recv()
        for step in range(1, n_sp):
            mixed = mixed + values_in[lax.rem(me + step, n_sp)][:, :head_dim]
        return mixed

    for layer in range(n_layers):
        sliding = layer < n_layers - 1
        slot = layer % 2
        res32 = residual.astype(F32)
        mean = jnp.sum(jnp.sum(res32, axis=1, keepdims=True), axis=0, keepdims=True) / dim
        centered = res32 - mean
        variance = jnp.sum(jnp.sum(centered * centered, axis=1, keepdims=True), axis=0, keepdims=True) / dim
        scaled = centered * lax.rsqrt(variance + NORM_EPS)
        for b in range(blocks):
            cols = slice(b * LANES, (b + 1) * LANES)
            line = scaled[b:b + 1, :] * gain_ref[layer:layer + 1, cols].astype(F32)
            normed[:, cols] = jnp.broadcast_to(line, (SUBLANES, LANES)).astype(BF16)
        waits = first_weights if layer == 0 else weight_copies(layer)
        waits[0].wait()

        @pl.loop(0, q_width // TILE)
        def _(n):
            cols = pl.ds(pl.multiple_of(n * TILE, TILE), TILE)
            query[:, cols] = jnp.dot(normed[...], wq[slot, :, cols], preferred_element_type=F32)

        q_wide = attention_query(layer, sliding)
        q_heads = q_wide[:, :head_dim]
        if layer == 0:
            queries[me] = q_wide.astype(F32)
            sent = messages(0, lambda dst: queries.at[me], queries.at[me])
            all_messages.extend(sent)
            start_bulk(*bulk_order[1])
            for copy in local_copies + first_weights[3:]:
                copy.start()
        waits[1].wait()
        k_col = contract_lanes(wk[slot], normed[...])
        if sliding:
            first, second = k_col[:half], k_col[half:]
            k_col = jnp.concatenate([first * cos_col[:half] - second * sin_col[:half], second * cos_col[half:] + first * sin_col[half:]], axis=0)
        waits[2].wait()
        v_col = contract_lanes(wv[slot], normed[...])
        columns = (k_col[:, 0:1].astype(BF16), v_col[:, 0:1].astype(BF16))
        if layer == 0:
            first_columns = columns
            v_row = contract_lanes(normed[...], wv[slot]).astype(BF16).astype(F32)
            mixed = spread_attention(q_heads, columns[0], v_row, sent)
        waits[3].wait()
        waits[4].wait()

        def gate_up(cols):
            gate = jnp.dot(normed[...], wg[slot, :, cols], preferred_element_type=F32)
            up = jnp.dot(normed[...], wu[slot, :, cols], preferred_element_type=F32)
            act[:, cols] = (gate * (1.0 / (1.0 + jnp.exp(-gate))) * up).astype(BF16)

        @pl.loop(0, ffn // TILE)
        def _(n):
            gate_up(pl.ds(pl.multiple_of(n * TILE, TILE), TILE))

        if ffn % TILE:
            gate_up(slice(ffn // TILE * TILE, ffn))
        waits[5].wait()

        @pl.loop(0, dim // TILE)
        def _(n):
            cols = pl.ds(pl.multiple_of(n * TILE, TILE), TILE)
            down = jnp.dot(act[...], wd[slot, :, cols], preferred_element_type=F32)
            mlp[:, cols] = down[0:1]

        if layer > 0:
            scores = []
            for part, keys in pieces(layer, 0, columns):
                score = jnp.dot(q_heads, keys, preferred_element_type=F32) * head_dim ** -0.5
                if not sliding:
                    ids = part * piece + lax.broadcasted_iota(jnp.int32, score.shape, 1)
                    score = jnp.where(ids <= my_len, score, -1e30)
                scores.append(score)
            top = functools.reduce(jnp.maximum, [jnp.max(score, axis=1, keepdims=True) for score in scores])
            scores = [jnp.exp(score - top) for score in scores]
            share = 1.0 / functools.reduce(jnp.add, [jnp.sum(score, axis=1, keepdims=True) for score in scores])
            weights = [(score * share).astype(BF16) for score in scores]
            mixed = functools.reduce(jnp.add, [contract_lanes(weight, values) for weight, (part, values) in zip(weights, pieces(layer, 1, columns))])
        mixed = jnp.where(own_head, jnp.concatenate([mixed] * n_heads, axis=1), 0.0)
        mixed = jnp.broadcast_to(jnp.sum(mixed, axis=0, keepdims=True), mixed.shape).astype(BF16)
        waits[6].wait()
        for n in range(dim // TILE):
            attn = jnp.dot(mixed, wo[slot, :, n * TILE:(n + 1) * TILE], preferred_element_type=F32)
            for b in range(n * TILE // LANES, (n + 1) * TILE // LANES):
                inner = slice(b * LANES - n * TILE, (b + 1) * LANES - n * TILE)
                sums[layer, my_tp, b:b + 1, :] = attn[0:1, inner] + mlp[:, b * LANES:(b + 1) * LANES]
        if layer + 2 < n_layers:
            for copy in weight_copies(layer + 2):
                copy.start()
        reduces = [pltpu.make_async_remote_copy(
            src_ref=sums.at[layer, my_tp], dst_ref=sums.at[layer, my_tp],
            send_sem=sum_send_sem.at[layer, step], recv_sem=sum_recv_sem.at[layer, step],
            device_id={"tp": lax.rem(my_tp + step, n_tp)}, device_id_type=MESH) for step in range(1, n_tp)]
        if layer == 0:
            @pl.when(jnp.logical_not(lead))
            def _():
                pl.semaphore_wait(ready_sem, 1)

        for copy in reduces:
            copy.start()
        for copy in reduces:
            copy.wait_recv()
        summed = res32
        for other in range(n_tp):
            summed = summed + sums[layer, other]
        residual = summed.astype(BF16)
        for copy in reduces:
            copy.wait_send()

    for b in range(blocks):
        hid_out[0:1, b * LANES:(b + 1) * LANES] = residual[b:b + 1, :]
    for kv in range(2):
        for _ in pieces(0, kv, first_columns):
            pass
    for copy in all_messages:
        copy.wait_send()
    for layer in range(n_layers):
        for kv in range(2):
            for copy in sends(layer, kv):
                copy.wait_send()


def solution(mesh):
    cache_spec = P(None, "dp", "tp", "sp", None)
    row_spec = P(("dp", "sp"), None)
    col_spec = P(None, None, "tp")
    inner_spec = P(None, "tp", None)
    window_spec = P(None, ("dp", "sp"), "tp", None, None)
    global_spec = P(("dp", "sp"), "tp", None, None)
    in_specs = (cache_spec, cache_spec, P("dp"), row_spec, P(None, None), col_spec, col_spec, col_spec, inner_spec, col_spec, col_spec, inner_spec)
    out_specs = (row_spec, window_spec, window_spec, global_spec, global_spec)
    n_sp, n_tp = mesh.shape["sp"], mesh.shape["tp"]

    def device_step(k_cache, v_cache, lengths, hidden, ln_gain, w_query, w_key, w_value, w_out, w_gate, w_up, w_down):
        n_layers, dim, q_width = w_query.shape
        n_rows, _, piece, head_dim = k_cache.shape[1:]
        ffn = w_gate.shape[-1]
        seq_len = piece * n_sp
        cache_k = jnp.swapaxes(k_cache, 3, 4).reshape(n_layers, n_rows, head_dim, piece)
        cache_v = jnp.swapaxes(v_cache, 3, 4).reshape(n_layers, n_rows, head_dim, piece)
        half = head_dim // 2
        freq = np.float32(1.0) / np.power(np.float32(ROPE_BASE), np.arange(half, dtype=np.float32) * np.float32(2.0) / np.float32(head_dim))
        freq_row = np.tile(freq.astype(np.float32), (SUBLANES, q_width // half))
        freq_col = np.tile(freq.astype(np.float32)[:, None], (2, SUBLANES))
        vmem = pl.BlockSpec(memory_space=pltpu.VMEM)
        hbm = pl.BlockSpec(memory_space=pl.ANY)
        shapes = [(1, dim)] + [(n_layers - 1, head_dim, WINDOW)] * 2 + [(head_dim, seq_len)] * 2
        results = pl.pallas_call(
            functools.partial(decode_kernel, n_sp, n_tp),
            out_shape=[pltpu.VMEM(shape, BF16) for shape in shapes],
            in_specs=[hbm] * 14,
            out_specs=[vmem] * len(shapes),
            scratch_shapes=[
                pltpu.VMEM((n_layers, 2, n_sp, head_dim, piece), BF16),
                pltpu.VMEM((2, dim, q_width), BF16),
                pltpu.VMEM((2, head_dim, dim), BF16),
                pltpu.VMEM((2, head_dim, dim), BF16),
                pltpu.VMEM((2, q_width, dim), BF16),
                pltpu.VMEM((2, dim, ffn), BF16),
                pltpu.VMEM((2, dim, ffn), BF16),
                pltpu.VMEM((2, ffn, dim), BF16),
                pltpu.VMEM((SUBLANES, dim), BF16),
                pltpu.VMEM((SUBLANES, q_width), F32),
                pltpu.VMEM((SUBLANES, ffn), BF16),
                pltpu.VMEM((1, dim), F32),
                pltpu.VMEM((n_layers, n_tp, dim // LANES, LANES), F32),
                pltpu.SMEM(lengths.shape, jnp.int32),
                pltpu.VMEM(hidden.shape, BF16),
                pltpu.VMEM(ln_gain.shape, BF16),
                pltpu.VMEM(freq_row.shape, F32),
                pltpu.VMEM(freq_col.shape, F32),
                pltpu.VMEM((2, n_rows, head_dim, piece), BF16),
                pltpu.VMEM((n_rows, SUBLANES, piece), F32),
                pltpu.VMEM((n_sp, SUBLANES, LANES), F32),
                pltpu.VMEM((n_sp, 2, SUBLANES, LANES), F32),
                pltpu.VMEM((n_sp, SUBLANES, LANES), F32),
                pltpu.VMEM((n_sp, SUBLANES, LANES), F32),
                pltpu.SemaphoreType.DMA((n_layers, 2, n_sp)),
                pltpu.SemaphoreType.DMA((n_layers, 2, n_sp)),
                pltpu.SemaphoreType.DMA((n_layers, 2)),
                pltpu.SemaphoreType.DMA((2, 7)),
                pltpu.SemaphoreType.DMA((5,)),
                pltpu.SemaphoreType.DMA((n_layers, n_tp)),
                pltpu.SemaphoreType.DMA((n_layers, n_tp)),
                pltpu.SemaphoreType.DMA((2,)),
                pltpu.SemaphoreType.DMA((3, n_sp)),
                pltpu.SemaphoreType.DMA((3, n_sp)),
                pltpu.SemaphoreType.REGULAR,
                pltpu.SemaphoreType.REGULAR,
            ],
            compiler_params=pltpu.CompilerParams(collective_id=0, has_side_effects=True, vmem_limit_bytes=55 << 20),
        )(lengths, hidden, ln_gain, freq_row, freq_col, cache_k, cache_v, w_query, jnp.swapaxes(w_key, 1, 2), jnp.swapaxes(w_value, 1, 2), w_out, w_gate, w_up, w_down)

        hid, win_k, win_v, glob_k, glob_v = pl.pallas_call(
            write_kernel,
            out_shape=[jax.ShapeDtypeStruct(shape, BF16) for shape in shapes],
            in_specs=[vmem] * len(shapes),
            out_specs=[hbm] * len(shapes),
            scratch_shapes=[pltpu.SemaphoreType.DMA((len(shapes),))],
            compiler_params=pltpu.CompilerParams(vmem_limit_bytes=1 << 20),
        )(*[pltpu.with_memory_space_constraint(result, pltpu.VMEM) for result in results])

        def back(array):
            lead = array.shape[:-2]
            return jnp.swapaxes(array.reshape(lead + (1, 1) + array.shape[-2:]), -2, -1)

        return hid, back(win_k), back(win_v), back(glob_k), back(glob_v)

    return jax.shard_map(device_step, mesh=mesh, in_specs=in_specs, out_specs=out_specs, check_vma=False)
```

```python
import functools

import jax
import jax.numpy as jnp
import numpy as np
from jax import lax
from jax.experimental import pallas as pl
from jax.experimental.pallas import tpu as pltpu
from jax.sharding import PartitionSpec as P

WINDOW = 4096
ROPE_BASE = 50000
NORM_EPS = 1e-5
LANES = 128
SUBLANES = 8
TILE = 256
CORES = 2
F32 = jnp.float32
BF16 = jnp.bfloat16
MESH = pl.DeviceIdType.MESH


def contract_lanes(left, right):
    return lax.dot_general(left, right, (((1,), (1,)), ((), ())), preferred_element_type=F32)


def write_kernel(*refs):
    count = (len(refs) - 1) // 2
    sources, targets, sem = refs[:count], refs[count:2 * count], refs[-1]
    copies = [pltpu.make_async_copy(src, dst, sem.at[i]) for i, (src, dst) in enumerate(zip(sources, targets))]
    for copy in copies:
        copy.start()
    for copy in copies:
        copy.wait()


def decode_kernel(n_sp, n_tp, len_in, hid_in, gain_in, freq_row_in, freq_col_in, k_ref, v_ref, wq_ref, wk_ref, wv_ref, wo_ref, wg_ref, wu_ref, wd_ref,
                  hid_out, win_k_out, win_v_out, glob_k_out, glob_v_out,
                  stage, wq, wk, wv, wo, wg, wu, wd, normed, query, act, mlp, sums, len_ref, hid_ref, gain_ref, freq_row_ref, freq_col_ref,
                  local, local_score, queries, stats, values_out, values_in,
                  send_sem, recv_sem, own_sem, weight_sem, small_sem, sum_send_sem, sum_recv_sem, local_sem, message_send_sem, message_recv_sem, line_sem, ready_sem):
    n_layers = wq_ref.shape[0]
    piece = k_ref.shape[-1]
    head_dim = k_ref.shape[-2]
    q_width = wq_ref.shape[-1]
    ffn = wg_ref.shape[-1]
    dim = wq_ref.shape[1]
    n_heads = q_width // head_dim
    half = head_dim // 2
    blocks = dim // LANES
    n_low = WINDOW // piece
    me = lax.axis_index("sp")
    my_tp = lax.axis_index("tp")

    weight_pairs = ((wq_ref, wq), (wk_ref, wk), (wv_ref, wv), (wg_ref, wg), (wu_ref, wu), (wd_ref, wd), (wo_ref, wo))

    def weight_copies(layer):
        slot = layer % 2
        return [pltpu.make_async_copy(src.at[layer], dst.at[slot], weight_sem.at[slot, i]) for i, (src, dst) in enumerate(weight_pairs)]

    barrier = pltpu.get_barrier_semaphore()
    for step in range(1, n_sp):
        pl.semaphore_signal(barrier, inc=1, device_id={"sp": lax.rem(me + step, n_sp)}, device_id_type=MESH)
    lead = me == 0

    @pl.when(lead)
    def _():
        for step in range(1, n_tp):
            pl.semaphore_signal(barrier, inc=1, device_id={"tp": lax.rem(my_tp + step, n_tp)}, device_id_type=MESH)
        pl.semaphore_wait(barrier, n_sp + n_tp - 2)

    @pl.when(jnp.logical_not(lead))
    def _():
        pl.semaphore_wait(barrier, n_sp - 1)

    chips = n_sp // CORES
    chip, core = lax.div(me, CORES), lax.rem(me, CORES)
    far_first = sorted(range(1, chips), key=lambda d: -min(d, chips - d))
    chip_order = [0] + far_first
    deltas = [(dc, dk) for dc in chip_order for dk in range(CORES) if (dc, dk) != (0, 0)]

    def shifted(dc, dk):
        return lax.rem(chip + dc, chips) * CORES + lax.rem(core + dk, CORES)

    def send(layer, kv, dc, dk):
        src = k_ref if kv == 0 else v_ref
        dst = shifted(dc, dk)
        at = dc * CORES + dk
        return pltpu.make_async_remote_copy(
            src_ref=src.at[layer, dst], dst_ref=stage.at[layer, kv, me],
            send_sem=send_sem.at[layer, kv, at], recv_sem=recv_sem.at[layer, kv, at],
            device_id={"sp": dst}, device_id_type=MESH)

    def sends(layer, kv):
        return [send(layer, kv, dc, dk) for dc, dk in deltas]

    def own_copy(layer, kv):
        src = k_ref if kv == 0 else v_ref
        return pltpu.make_async_copy(src.at[layer, me], stage.at[layer, kv, me], own_sem.at[layer, kv])

    def start_bulk(layer, kv):
        for copy in sends(layer, kv):
            copy.start()
        own_copy(layer, kv).start()

    bulk_order = [(layer, kv) for layer in list(range(1, n_layers)) + [0] for kv in range(2)]
    start_bulk(*bulk_order[0])
    small_pairs = ((len_in, len_ref), (hid_in, hid_ref), (gain_in, gain_ref), (freq_row_in, freq_row_ref), (freq_col_in, freq_col_ref))
    small_copies = [pltpu.make_async_copy(src, dst, small_sem.at[i]) for i, (src, dst) in enumerate(small_pairs)]
    local_copies = [pltpu.make_async_copy(src.at[0], local.at[kv], local_sem.at[kv]) for kv, src in enumerate((k_ref, v_ref))]
    first_weights = weight_copies(0)
    for copy in small_copies + first_weights[:3]:
        copy.start()

    @pl.when(lead)
    def _():
        for step in range(1, n_tp):
            pl.semaphore_signal(line_sem, inc=1, device_id={"tp": lax.rem(my_tp + step, n_tp)}, device_id_type=MESH)
        pl.semaphore_wait(line_sem, n_tp - 1)
        for step in range(1, n_sp):
            pl.semaphore_signal(ready_sem, inc=1, device_id={"sp": lax.rem(me + step, n_sp)}, device_id_type=MESH)

    for copy in small_copies:
        copy.wait()

    def messages(kind, source, target):
        found = []
        for step in range(1, n_sp):
            dst = lax.rem(me + step, n_sp)
            found.append(pltpu.make_async_remote_copy(
                src_ref=source(dst), dst_ref=target,
                send_sem=message_send_sem.at[kind, step], recv_sem=message_recv_sem.at[kind, step],
                device_id={"sp": dst}, device_id_type=MESH))
        for copy in found:
            copy.start()
        return found

    def wait_from(layer, kv, dc, dk):
        if (dc, dk) == (0, 0):
            own_copy(layer, kv).wait()
        else:
            send(layer, kv, (chips - dc) % chips, dk).wait_recv()

    my_len = len_ref[me]
    last_slot = my_len - WINDOW
    angle_row = my_len.astype(F32) * freq_row_ref[...]
    cos_row = jnp.cos(angle_row)
    sin_row = jnp.sin(angle_row)
    angle_col = my_len.astype(F32) * freq_col_ref[...]
    cos_col = jnp.cos(angle_col)
    sin_col = jnp.sin(angle_col)
    lane_q = lax.broadcasted_iota(jnp.int32, (SUBLANES, q_width), 1)
    row_q = lax.broadcasted_iota(jnp.int32, (SUBLANES, q_width), 0)
    first_half = lax.rem(lane_q, head_dim) < half
    own_head = lax.div(lane_q, head_dim) == row_q

    residual = jnp.concatenate([hid_ref[0:1, b * LANES:(b + 1) * LANES] for b in range(blocks)], axis=0)

    lane_t = lax.broadcasted_iota(jnp.int32, (SUBLANES, LANES), 1)
    sublane_t = lax.broadcasted_iota(jnp.int32, (SUBLANES, LANES), 0)
    middle = SUBLANES * n_sp
    all_messages = []

    def attention_query(sliding):
        q = query[...]
        if sliding:
            partner = jnp.where(first_half, pltpu.roll(q, q_width - half, 1), pltpu.roll(q, half, 1))
            q = q * cos_row + jnp.where(first_half, -partner, partner) * sin_row
        return q.astype(BF16).astype(F32)

    def split_heads(q):
        q = jnp.where(own_head, q, 0.0)
        q = functools.reduce(lambda a, b: a + b, [q[:, b * LANES:(b + 1) * LANES] for b in range(q_width // LANES)])
        return (q[:, :head_dim] + q[:, head_dim:2 * head_dim]).astype(BF16)

    def flat_heads(heads):
        spread = jnp.where(own_head, jnp.concatenate([heads] * n_heads, axis=1), 0.0)
        return jnp.sum(spread, axis=0, keepdims=True)

    def flat_lanes(row, first):
        return lane_t == first + n_sp * sublane_t + row

    def pieces(layer, kv, columns):
        sliding = layer < n_layers - 1
        new = jnp.broadcast_to(columns[kv], (head_dim, piece))
        lanes = lax.broadcasted_iota(jnp.int32, (head_dim, piece), 1)
        if sliding:
            target = (win_k_out if kv == 0 else win_v_out).at[layer]
            half_chips = chips // 2
            for dc in sorted(range(half_chips)):
                for dk in range(CORES):
                    wait_from(layer, kv, dc, dk)
                    wait_from(layer, kv, dc + half_chips, dk)
                    part = lax.rem(shifted(dc, dk), n_low)
                    ids = part * piece + lanes
                    value = jnp.where(ids < last_slot, stage[layer, kv, part + n_low], stage[layer, kv, part])
                    value = jnp.where(ids == last_slot, new, value)
                    target[:, pl.ds(pl.multiple_of(part * piece, piece), piece)] = value
                    yield part, value
        else:
            target = glob_k_out if kv == 0 else glob_v_out
            for dc in chip_order:
                for dk in range(CORES):
                    wait_from(layer, kv, dc, dk)
                    part = shifted(dc, dk)
                    ids = part * piece + lanes
                    value = jnp.where(ids < my_len, stage[layer, kv, part], jnp.zeros_like(new))
                    value = jnp.where(ids == my_len, new, value)
                    target[:, pl.ds(pl.multiple_of(part * piece, piece), piece)] = value
                    yield part, value

    def spread_attention(q_heads, k_new, v_row, sent):
        for copy in sent:
            copy.wait_recv()
        local_copies[0].wait()
        positions = me * piece + lax.broadcasted_iota(jnp.int32, (SUBLANES, piece), 1)
        new_score = jnp.dot(q_heads, jnp.broadcast_to(k_new, (head_dim, LANES)), preferred_element_type=F32) * head_dim ** -0.5
        packed = jnp.zeros((SUBLANES, LANES), F32)
        for row in range(n_sp):
            row_heads = split_heads(jnp.broadcast_to(queries[row], (SUBLANES, q_width)))
            score = jnp.dot(row_heads, local[0, row], preferred_element_type=F32) * head_dim ** -0.5
            valid = (positions > len_ref[row] - WINDOW) & (positions < len_ref[row])
            score = jnp.where(valid, score, -1e30)
            local_score[row] = score
            top = jnp.max(score, axis=1, keepdims=True)
            norm = jnp.sum(jnp.exp(score - top), axis=1, keepdims=True)
            mine = me == row
            raised = jnp.where(mine, jnp.maximum(top, new_score[:, 0:1]), top)
            norm = norm * jnp.exp(top - raised) + jnp.where(mine, jnp.exp(jnp.minimum(new_score[:, 0:1] - raised, 0.0)), 0.0)
            packed = jnp.where(flat_lanes(row, 0), raised, packed)
            packed = jnp.where(flat_lanes(row, middle), norm, packed)
        stats[me] = jnp.sum(packed, axis=0, keepdims=True)
        sent = messages(1, lambda dst: stats.at[me], stats.at[me])
        all_messages.extend(sent)
        start_bulk(*bulk_order[2])
        for copy in weight_copies(1):
            copy.start()
        for copy in sent:
            copy.wait_recv()
        local_copies[1].wait()
        gathered = [jnp.broadcast_to(stats[src], (SUBLANES, LANES)) for src in range(n_sp)]
        low = lane_t < middle
        top = functools.reduce(jnp.maximum, gathered)
        norm = functools.reduce(jnp.add, [pltpu.roll(each, LANES - middle, 1) * jnp.exp(jnp.where(low, each - top, 0.0)) for each in gathered])
        share = 1.0 / jnp.where(low, norm, 1.0)

        def column(tile, row):
            return jnp.sum(jnp.where(flat_lanes(row, 0), tile, 0.0), axis=1, keepdims=True)

        for row in range(n_sp):
            weight = (jnp.exp(local_score[row] - column(top, row)) * column(share, row)).astype(BF16)
            values_out[row] = flat_heads(contract_lanes(weight, local[1, row]))
        sent = messages(2, lambda dst: values_out.at[dst], values_in.at[me])
        all_messages.extend(sent)
        for group in bulk_order[3:]:
            start_bulk(*group)
        new_weight = (jnp.exp(new_score[:, 0:1] - column(top, me)) * column(share, me)).astype(BF16).astype(F32)
        mixed = flat_heads(new_weight * v_row) + values_out[me]
        for copy in sent:
            copy.wait_recv()
        for step in range(1, n_sp):
            mixed = mixed + values_in[lax.rem(me + step, n_sp)]
        return mixed

    for layer in range(n_layers):
        sliding = layer < n_layers - 1
        slot = layer % 2
        res32 = residual.astype(F32)
        mean = jnp.sum(jnp.sum(res32, axis=1, keepdims=True), axis=0, keepdims=True) / dim
        centered = res32 - mean
        variance = jnp.sum(jnp.sum(centered * centered, axis=1, keepdims=True), axis=0, keepdims=True) / dim
        scaled = centered * lax.rsqrt(variance + NORM_EPS)
        for b in range(blocks):
            cols = slice(b * LANES, (b + 1) * LANES)
            line = scaled[b:b + 1, :] * gain_ref[layer:layer + 1, cols].astype(F32)
            normed[:, cols] = jnp.broadcast_to(line, (SUBLANES, LANES)).astype(BF16)
        waits = first_weights if layer == 0 else weight_copies(layer)
        waits[0].wait()

        @pl.loop(0, q_width // TILE)
        def _(n):
            cols = pl.ds(pl.multiple_of(n * TILE, TILE), TILE)
            query[:, cols] = jnp.dot(normed[...], wq[slot, :, cols], preferred_element_type=F32)

        q_wide = attention_query(sliding)
        q_heads = split_heads(q_wide)
        if layer == 0:
            queries[me] = q_wide[0:1]
            sent = messages(0, lambda dst: queries.at[me], queries.at[me])
            all_messages.extend(sent)
            start_bulk(*bulk_order[1])
            for copy in local_copies + first_weights[3:]:
                copy.start()
        waits[1].wait()
        k_col = contract_lanes(wk[slot], normed[...])
        if sliding:
            first, second = k_col[:half], k_col[half:]
            k_col = jnp.concatenate([first * cos_col[:half] - second * sin_col[:half], second * cos_col[half:] + first * sin_col[half:]], axis=0)
        waits[2].wait()
        v_col = contract_lanes(wv[slot], normed[...])
        columns = (k_col[:, 0:1].astype(BF16), v_col[:, 0:1].astype(BF16))
        if layer == 0:
            first_columns = columns
            v_row = contract_lanes(normed[...], wv[slot]).astype(BF16).astype(F32)
            mixed = spread_attention(q_heads, columns[0], v_row, sent)
        waits[3].wait()
        waits[4].wait()

        def gate_up(cols):
            gate = jnp.dot(normed[...], wg[slot, :, cols], preferred_element_type=F32)
            up = jnp.dot(normed[...], wu[slot, :, cols], preferred_element_type=F32)
            act[:, cols] = (gate * (1.0 / (1.0 + jnp.exp(-gate))) * up).astype(BF16)

        @pl.loop(0, ffn // TILE)
        def _(n):
            gate_up(pl.ds(pl.multiple_of(n * TILE, TILE), TILE))

        if ffn % TILE:
            gate_up(slice(ffn // TILE * TILE, ffn))
        waits[5].wait()

        @pl.loop(0, dim // TILE)
        def _(n):
            cols = pl.ds(pl.multiple_of(n * TILE, TILE), TILE)
            down = jnp.dot(act[...], wd[slot, :, cols], preferred_element_type=F32)
            mlp[:, cols] = down[0:1]

        if layer > 0:
            scores = []
            for part, keys in pieces(layer, 0, columns):
                score = jnp.dot(q_heads, keys, preferred_element_type=F32) * head_dim ** -0.5
                if not sliding:
                    ids = part * piece + lax.broadcasted_iota(jnp.int32, score.shape, 1)
                    score = jnp.where(ids <= my_len, score, -1e30)
                scores.append(score)
            top = functools.reduce(jnp.maximum, [jnp.max(score, axis=1, keepdims=True) for score in scores])
            scores = [jnp.exp(score - top) for score in scores]
            share = 1.0 / functools.reduce(jnp.add, [jnp.sum(score, axis=1, keepdims=True) for score in scores])
            weights = [(score * share).astype(BF16) for score in scores]
            mixed = flat_heads(functools.reduce(jnp.add, [contract_lanes(weight, values) for weight, (part, values) in zip(weights, pieces(layer, 1, columns))]))
        mixed = jnp.broadcast_to(mixed, (SUBLANES, q_width)).astype(BF16)
        waits[6].wait()
        for n in range(dim // TILE):
            attn = jnp.dot(mixed, wo[slot, :, n * TILE:(n + 1) * TILE], preferred_element_type=F32)
            for b in range(n * TILE // LANES, (n + 1) * TILE // LANES):
                inner = slice(b * LANES - n * TILE, (b + 1) * LANES - n * TILE)
                sums[layer, my_tp, b:b + 1, :] = attn[0:1, inner] + mlp[:, b * LANES:(b + 1) * LANES]
        if layer + 2 < n_layers:
            for copy in weight_copies(layer + 2):
                copy.start()
        reduces = [pltpu.make_async_remote_copy(
            src_ref=sums.at[layer, my_tp], dst_ref=sums.at[layer, my_tp],
            send_sem=sum_send_sem.at[layer, step], recv_sem=sum_recv_sem.at[layer, step],
            device_id={"tp": lax.rem(my_tp + step, n_tp)}, device_id_type=MESH) for step in range(1, n_tp)]
        if layer == 0:
            @pl.when(jnp.logical_not(lead))
            def _():
                pl.semaphore_wait(ready_sem, 1)

        for copy in reduces:
            copy.start()
        for copy in reduces:
            copy.wait_recv()
        summed = res32
        for other in range(n_tp):
            summed = summed + sums[layer, other]
        residual = summed.astype(BF16)
        for copy in reduces:
            copy.wait_send()

    for b in range(blocks):
        hid_out[0:1, b * LANES:(b + 1) * LANES] = residual[b:b + 1, :]
    for kv in range(2):
        for _ in pieces(0, kv, first_columns):
            pass
    for copy in all_messages:
        copy.wait_send()
    for layer in range(n_layers):
        for kv in range(2):
            for copy in sends(layer, kv):
                copy.wait_send()


def solution(mesh):
    cache_spec = P(None, "dp", "tp", "sp", None)
    row_spec = P(("dp", "sp"), None)
    col_spec = P(None, None, "tp")
    inner_spec = P(None, "tp", None)
    window_spec = P(None, ("dp", "sp"), "tp", None, None)
    global_spec = P(("dp", "sp"), "tp", None, None)
    in_specs = (cache_spec, cache_spec, P("dp"), row_spec, P(None, None), col_spec, col_spec, col_spec, inner_spec, col_spec, col_spec, inner_spec)
    out_specs = (row_spec, window_spec, window_spec, global_spec, global_spec)
    n_sp, n_tp = mesh.shape["sp"], mesh.shape["tp"]

    def device_step(k_cache, v_cache, lengths, hidden, ln_gain, w_query, w_key, w_value, w_out, w_gate, w_up, w_down):
        n_layers, dim, q_width = w_query.shape
        n_rows, _, piece, head_dim = k_cache.shape[1:]
        ffn = w_gate.shape[-1]
        seq_len = piece * n_sp
        cache_k = jnp.swapaxes(k_cache, 3, 4).reshape(n_layers, n_rows, head_dim, piece)
        cache_v = jnp.swapaxes(v_cache, 3, 4).reshape(n_layers, n_rows, head_dim, piece)
        half = head_dim // 2
        freq = np.float32(1.0) / np.power(np.float32(ROPE_BASE), np.arange(half, dtype=np.float32) * np.float32(2.0) / np.float32(head_dim))
        freq_row = np.tile(freq.astype(np.float32), (SUBLANES, q_width // half))
        freq_col = np.tile(freq.astype(np.float32)[:, None], (2, SUBLANES))
        vmem = pl.BlockSpec(memory_space=pltpu.VMEM)
        hbm = pl.BlockSpec(memory_space=pl.ANY)
        shapes = [(1, dim)] + [(n_layers - 1, head_dim, WINDOW)] * 2 + [(head_dim, seq_len)] * 2
        results = pl.pallas_call(
            functools.partial(decode_kernel, n_sp, n_tp),
            out_shape=[pltpu.VMEM(shape, BF16) for shape in shapes],
            in_specs=[hbm] * 14,
            out_specs=[vmem] * len(shapes),
            scratch_shapes=[
                pltpu.VMEM((n_layers, 2, n_sp, head_dim, piece), BF16),
                pltpu.VMEM((2, dim, q_width), BF16),
                pltpu.VMEM((2, head_dim, dim), BF16),
                pltpu.VMEM((2, head_dim, dim), BF16),
                pltpu.VMEM((2, q_width, dim), BF16),
                pltpu.VMEM((2, dim, ffn), BF16),
                pltpu.VMEM((2, dim, ffn), BF16),
                pltpu.VMEM((2, ffn, dim), BF16),
                pltpu.VMEM((SUBLANES, dim), BF16),
                pltpu.VMEM((SUBLANES, q_width), F32),
                pltpu.VMEM((SUBLANES, ffn), BF16),
                pltpu.VMEM((1, dim), F32),
                pltpu.VMEM((n_layers, n_tp, dim // LANES, LANES), F32),
                pltpu.SMEM(lengths.shape, jnp.int32),
                pltpu.VMEM(hidden.shape, BF16),
                pltpu.VMEM(ln_gain.shape, BF16),
                pltpu.VMEM(freq_row.shape, F32),
                pltpu.VMEM(freq_col.shape, F32),
                pltpu.VMEM((2, n_rows, head_dim, piece), BF16),
                pltpu.VMEM((n_rows, SUBLANES, piece), F32),
                pltpu.VMEM((n_sp, 1, q_width), F32),
                pltpu.VMEM((n_sp, 1, LANES), F32),
                pltpu.VMEM((n_sp, 1, q_width), F32),
                pltpu.VMEM((n_sp, 1, q_width), F32),
                pltpu.SemaphoreType.DMA((n_layers, 2, n_sp)),
                pltpu.SemaphoreType.DMA((n_layers, 2, n_sp)),
                pltpu.SemaphoreType.DMA((n_layers, 2)),
                pltpu.SemaphoreType.DMA((2, 7)),
                pltpu.SemaphoreType.DMA((5,)),
                pltpu.SemaphoreType.DMA((n_layers, n_tp)),
                pltpu.SemaphoreType.DMA((n_layers, n_tp)),
                pltpu.SemaphoreType.DMA((2,)),
                pltpu.SemaphoreType.DMA((3, n_sp)),
                pltpu.SemaphoreType.DMA((3, n_sp)),
                pltpu.SemaphoreType.REGULAR,
                pltpu.SemaphoreType.REGULAR,
            ],
            compiler_params=pltpu.CompilerParams(collective_id=0, has_side_effects=True, vmem_limit_bytes=55 << 20),
        )(lengths, hidden, ln_gain, freq_row, freq_col, cache_k, cache_v, w_query, jnp.swapaxes(w_key, 1, 2), jnp.swapaxes(w_value, 1, 2), w_out, w_gate, w_up, w_down)

        hid, win_k, win_v, glob_k, glob_v = pl.pallas_call(
            write_kernel,
            out_shape=[jax.ShapeDtypeStruct(shape, BF16) for shape in shapes],
            in_specs=[vmem] * len(shapes),
            out_specs=[hbm] * len(shapes),
            scratch_shapes=[pltpu.SemaphoreType.DMA((len(shapes),))],
            compiler_params=pltpu.CompilerParams(vmem_limit_bytes=1 << 20),
        )(*[pltpu.with_memory_space_constraint(result, pltpu.VMEM) for result in results])

        def back(array):
            lead = array.shape[:-2]
            return jnp.swapaxes(array.reshape(lead + (1, 1) + array.shape[-2:]), -2, -1)

        return hid, back(win_k), back(win_v), back(glob_k), back(glob_v)

    return jax.shard_map(device_step, mesh=mesh, in_specs=in_specs, out_specs=out_specs, check_vma=False)
```
